32 devices in a mesh: ctx: 16 (over z, x, core), head: 2 (over y).
Axes of the slice: x: 2, y: 2, z: 4, core: 2. Of those that a mesh axis runs over, the one named last changes fastest.
Arguments:
- queries: bfloat16 [256, 4096], P('ctx', 'head'), may hold values from -1500 to 1500
- cache_keys: bfloat16 [65536, 2048], P('ctx', 'head'), may hold values from -15 to 15
- prefix_cache_values: bfloat16 [65536, 2048], P('ctx', 'head'), may hold values from -6 to 6
- incoming_keys: bfloat16 [256, 2048], P('ctx', 'head'), may hold values from -15 to 15
- incoming_values: bfloat16 [256, 2048], P('ctx', 'head'), may hold values from -6 to 6
Outputs:
- attended: bfloat16 [256, 4096], P('ctx', 'head')
The draws below stay inside these ranges and needn't reach their ends.
All inputs are finite; a program needn't handle non-finite values.
Results may differ from the reference program's by a relative error of at most 0.005.
Values may be sent and summed in bfloat16 or wider, within the bound.
A program may use at most 64 MiB of HBM per device.

```python
import jax
import jax.numpy as jnp
from jax import lax

QUERY_HEAD_COUNT = 32
KEY_VALUE_HEADS = 16
HEAD_SIZE = 128
PREFIX_TOKENS = 65536
NEW_TOKEN_COUNT = 256


def chosen_pairs(key):
    picker = jax.random.fold_in(key, 12)
    first = jax.random.randint(jax.random.fold_in(picker, 1), (16,), 0, PREFIX_TOKENS)
    second = (first + PREFIX_TOKENS // 2) % PREFIX_TOKENS
    query_rows = jax.random.randint(jax.random.fold_in(picker, 2), (16,), 0, NEW_TOKEN_COUNT)
    current_query_head = jax.random.randint(jax.random.fold_in(picker, 3), (16,), 0, QUERY_HEAD_COUNT)
    strength = jax.random.uniform(jax.random.fold_in(picker, 4), (16,), jnp.float32, 1.8, 4.5)
    return (first, second, query_rows, current_query_head, strength)


def base_keys(key):
    sampled_inputs = 2.5 * jax.random.truncated_normal(jax.random.fold_in(key, 11), -6.0, 6.0, (PREFIX_TOKENS, KEY_VALUE_HEADS * HEAD_SIZE), jnp.float32)
    first, second, query_rows, current_query_head, strength = chosen_pairs(key)
    sampled_inputs = sampled_inputs.at[second].set(0.99 * sampled_inputs[first])
    return sampled_inputs


def draw_cache_keys(key, part):
    return base_keys(key).astype(jnp.bfloat16)


def draw_queries(key, part):
    sampled_inputs = jax.random.truncated_normal(jax.random.fold_in(key, 13), -6.0, 6.0, (NEW_TOKEN_COUNT, QUERY_HEAD_COUNT * HEAD_SIZE), jnp.float32)
    key_table = base_keys(key).astype(jnp.bfloat16).astype(jnp.float32)
    first, second, query_rows, current_query_head, strength = chosen_pairs(key)
    key_value_head = current_query_head // (QUERY_HEAD_COUNT // KEY_VALUE_HEADS)
    offsets = jnp.arange(HEAD_SIZE, dtype=jnp.int32)
    key_cols = key_value_head[:, None] * HEAD_SIZE + offsets[None, :]
    picked = key_table[first[:, None], key_cols] * strength[:, None]
    query_cols = current_query_head[:, None] * HEAD_SIZE + offsets[None, :]
    sampled_inputs = sampled_inputs.at[query_rows[:, None], query_cols].set(picked)
    return sampled_inputs.astype(jnp.bfloat16)


def levels(own_key, dims, shards, least, largest):
    gain, own = 1.0, jax.random.fold_in(own_key, 6)
    for dim, parts in shards:
        steps = jnp.exp(jax.random.uniform(jax.random.fold_in(own, dim), (parts,), jnp.float32, least / len(shards), largest / len(shards)))
        gain = gain * jnp.repeat(steps, dims[dim] // parts).reshape([-1 if axis == dim else 1 for axis in range(len(dims))])
    return gain


def scatter_about(rng, extent, spread, bound, shards=(), kind=jnp.bfloat16):
    drawn = jax.random.normal(rng, extent, jnp.float32) * spread
    if len(shards) > 0:
        drawn = levels(rng, extent, shards, -0.22, 0.18) * drawn
    return jnp.clip(drawn, min=-bound, max=bound).astype(kind)


def setup_inputs(seed: int = 0) -> dict:
    splits = jax.random.split(jax.random.key(seed), 6)
    return {
        "queries": draw_queries(jax.random.fold_in(splits[5], 71), 0),
        "cache_keys": draw_cache_keys(jax.random.fold_in(splits[5], 71), 0),
        "prefix_cache_values": scatter_about(splits[2], (PREFIX_TOKENS, KEY_VALUE_HEADS * HEAD_SIZE), 1.0, 6.0, ((0, 16), (1, 2))),
        "incoming_keys": scatter_about(splits[3], (NEW_TOKEN_COUNT, KEY_VALUE_HEADS * HEAD_SIZE), 2.5, 15.0, ((0, 16), (1, 2))),
        "incoming_values": scatter_about(splits[4], (NEW_TOKEN_COUNT, KEY_VALUE_HEADS * HEAD_SIZE), 1.0, 6.0, ((0, 16), (1, 2))),
    }


score_scale = 168.0 ** -0.5


def prefix_step(state, key_block, query_heads):
    out_acc, row_max, row_sum = state
    block_keys, block_values = key_block
    scores = jnp.einsum("gqd,kd->gqk", query_heads.astype(jnp.float32), block_keys.astype(jnp.float32)) * score_scale
    new_max = jnp.maximum(row_max, jnp.max(scores, axis=-1))
    decay = jnp.exp(row_max - new_max)
    probs = jnp.exp(scores - new_max[..., None])
    row_sum = row_sum * decay + jnp.sum(probs, axis=-1)
    rounded = lax.optimization_barrier(probs.astype(jnp.bfloat16)).astype(jnp.float32)
    out_acc = out_acc * decay[..., None] + jnp.einsum("gqk,kd->gqd", rounded, block_values.astype(jnp.float32))
    return (out_acc, new_max, row_sum), None


def one_head(operands):
    query_heads, head_keys, head_values, fresh_keys, fresh_values = operands
    group_size, total_rows, _ = query_heads.shape
    block_size = min(512, head_keys.shape[0])
    count = head_keys.shape[0] // block_size
    blocks = (head_keys.reshape(count, block_size, HEAD_SIZE), head_values.reshape(count, block_size, HEAD_SIZE))
    init = (jnp.zeros((group_size, total_rows, HEAD_SIZE), jnp.float32),
            jnp.full((group_size, total_rows), -1e30, jnp.float32),
            jnp.zeros((group_size, total_rows), jnp.float32))
    (out_acc, row_max, row_sum), _ = lax.scan(lambda state, key_block: prefix_step(state, key_block, query_heads), init, blocks)
    scores = jnp.einsum("gqd,kd->gqk", query_heads.astype(jnp.float32), fresh_keys.astype(jnp.float32)) * score_scale
    positions = jnp.arange(total_rows, dtype=jnp.int32)
    causal_mask = positions[None, :] <= positions[:, None]
    scores = jnp.where(causal_mask[None], scores, -1e30)
    fresh_max = jnp.max(scores, axis=-1)
    fresh_probs = jnp.where(causal_mask[None], jnp.exp(scores - fresh_max[..., None]), 0.0)
    fresh_sum = jnp.sum(fresh_probs, axis=-1)
    rounded = lax.optimization_barrier(fresh_probs.astype(jnp.bfloat16)).astype(jnp.float32)
    fresh_out = jnp.einsum("gqk,kd->gqd", rounded, fresh_values.astype(jnp.float32))
    merged_max = jnp.maximum(row_max, fresh_max)
    old_weight = jnp.exp(row_max - merged_max)
    new_weight = jnp.exp(fresh_max - merged_max)
    numer = out_acc * old_weight[..., None] + fresh_out * new_weight[..., None]
    denom = row_sum * old_weight + fresh_sum * new_weight
    return (numer / denom[..., None]).astype(jnp.bfloat16)


def reference(queries, cache_keys, prefix_cache_values, incoming_keys, incoming_values):
    total_rows = queries.shape[0]
    kv_heads = cache_keys.shape[1] // HEAD_SIZE
    group_size = queries.shape[1] // cache_keys.shape[1]
    query_heads = queries.reshape(total_rows, kv_heads, group_size, HEAD_SIZE).transpose(1, 2, 0, 3)
    head_keys = cache_keys.reshape(-1, kv_heads, HEAD_SIZE).transpose(1, 0, 2)
    head_values = prefix_cache_values.reshape(-1, kv_heads, HEAD_SIZE).transpose(1, 0, 2)
    fresh_keys = incoming_keys.reshape(total_rows, kv_heads, HEAD_SIZE).transpose(1, 0, 2)
    fresh_values = incoming_values.reshape(total_rows, kv_heads, HEAD_SIZE).transpose(1, 0, 2)
    outputs = lax.map(one_head, (query_heads, head_keys, head_values, fresh_keys, fresh_values))
    return outputs.transpose(2, 0, 1, 3).reshape(total_rows, -1)
```

```python
import functools
import math

import jax
import jax.numpy as jnp
from jax import lax
from jax.experimental import pallas as pl
from jax.experimental.pallas import tpu as pltpu
from jax.sharding import PartitionSpec as P

HEAD_SIZE = 128
LANES = 128
BLOCK_KEYS = 512
EXP2_SCALE = 168.0 ** (-0.5) * math.log2(math.e)
MASKED = -1e30


def nt_dot(a, b):
    return lax.dot_general(a, b, (((1,), (1,)), ((), ())), preferred_element_type=jnp.float32)


def kernel(
    devices, heads, group, own, block,
    q_hbm, k_hbm, v_hbm, fk_hbm, fv_hbm, out_ref,
    qbuf, kbuf, vbuf, fkbuf, fvbuf, scores, fresh_scores, visible,
    part_max, full_max, part_sum, acc, obuf, rbuf, mlbuf, rmlbuf,
    q_sem, k_sem, v_sem, fk_sem, fv_sem,
    gather_send, gather_recv, relay_send, relay_recv,
    o_send, o_recv, ml_send, ml_recv,
):
    pairs = devices // 2
    each = group * own
    rows = devices * each
    count = kbuf.shape[1] // block
    me = lax.axis_index("ctx")
    core, pair = lax.rem(me, 2), lax.div(me, 2)
    my_slot = core * pairs + pair

    def q_copy(h, g):
        columns = pl.ds((h * group + g) * HEAD_SIZE, HEAD_SIZE)
        return pltpu.make_async_copy(
            q_hbm.at[:, columns], qbuf.at[h, core, pair, pl.ds(g * own, own)], q_sem.at[h, g]
        )

    def head_columns(h):
        return pl.ds(pl.multiple_of(h * HEAD_SIZE, HEAD_SIZE), HEAD_SIZE)

    def k_copy(h):
        return pltpu.make_async_copy(k_hbm.at[:, head_columns(h)], kbuf.at[h], k_sem.at[h])

    def v_copy(h):
        return pltpu.make_async_copy(v_hbm.at[:, head_columns(h)], vbuf.at[h], v_sem.at[h])

    def fk_copy(h):
        return pltpu.make_async_copy(
            fk_hbm.at[:, head_columns(h)], fkbuf.at[h, pl.ds(0, own)], fk_sem.at[h]
        )

    def fv_copy(h):
        return pltpu.make_async_copy(
            fv_hbm.at[:, head_columns(h)], fvbuf.at[h, pl.ds(0, own)], fv_sem.at[h]
        )

    for h in range(heads):
        for g in range(group):
            q_copy(h, g).start()

    barrier = pltpu.get_barrier_semaphore()

    def greet(step, _):
        peer = lax.rem(me + step, devices)
        pl.semaphore_signal(
            barrier, inc=1, device_id={"ctx": peer}, device_id_type=pl.DeviceIdType.MESH
        )
        return 0

    lax.fori_loop(1, devices, greet, 0)
    fkbuf[:, own:, :] = jnp.zeros((heads, LANES - own, HEAD_SIZE), fkbuf.dtype)
    fvbuf[:, own:, :] = jnp.zeros((heads, LANES - own, HEAD_SIZE), fvbuf.dtype)
    for h in range(heads):
        fk_copy(h).start()
        k_copy(h).start()
        fv_copy(h).start()
        v_copy(h).start()

    key_lane = lax.broadcasted_iota(jnp.int32, (own, LANES), 1)
    key_pos = me * own + key_lane
    token = lax.broadcasted_iota(jnp.int32, (own, LANES), 0)
    for slot in range(devices):
        device = (slot % pairs) * 2 + slot // pairs
        seen = jnp.where((key_lane < own) & (key_pos <= device * own + token), 0.0, MASKED)
        for g in range(group):
            visible[pl.ds(slot * each + g * own, own), :] = seen

    for h in range(heads):
        for g in range(group):
            q_copy(h, g).wait()
    pl.semaphore_wait(barrier, devices - 1)

    def gather_copy(h, peer_pair):
        mine = qbuf.at[h, core, pair]
        return pltpu.make_async_remote_copy(
            src_ref=mine, dst_ref=mine, send_sem=gather_send.at[h], recv_sem=gather_recv.at[h],
            device_id={"ctx": peer_pair * 2 + core}, device_id_type=pl.DeviceIdType.MESH,
        )

    def gather_head(h, _):
        def send(step, _):
            gather_copy(h, lax.rem(pair + step, pairs)).start()
            return 0

        return lax.fori_loop(1, pairs, send, 0)

    lax.fori_loop(0, heads, gather_head, 0)

    def relay_copy(h):
        mine = qbuf.at[h, core]
        return pltpu.make_async_remote_copy(
            src_ref=mine, dst_ref=mine, send_sem=relay_send.at[h], recv_sem=relay_recv.at[h],
            device_id={"ctx": pair * 2 + 1 - core}, device_id_type=pl.DeviceIdType.MESH,
        )

    def gather_blocks(h, sem):
        blocks = qbuf.at[h, core, pl.ds(0, pairs - 1)]
        return pltpu.make_async_copy(blocks, blocks, sem.at[h])

    def relay(h):
        gather_blocks(h, gather_recv).wait()
        relay_copy(h).start()

    def queries_of(h):
        return qbuf[h].reshape(rows, HEAD_SIZE)

    def scores_open(h):
        relay_copy(h).wait_recv()
        fk_copy(h).wait()
        k_copy(h).wait()
        s = nt_dot(queries_of(h), fkbuf[h]) + visible[...]
        s = jnp.where(visible[...] < 0.0, MASKED, s)
        fresh_scores[lax.rem(h, 2)] = s
        part_max[...] = s

    def scores_block(h, c):
        keys = kbuf[h, pl.ds(pl.multiple_of(c * block, block), block), :]
        s = nt_dot(queries_of(h), keys)
        scores[lax.rem(h, 2), c] = s
        top = part_max[...]
        for i in range(block // LANES):
            top = jnp.maximum(top, s[:, i * LANES:(i + 1) * LANES])
        part_max[...] = top

    def scores_close():
        full_max[...] = jnp.broadcast_to(
            jnp.max(part_max[...], axis=1, keepdims=True), full_max.shape
        )

    def values_open(h):
        fv_copy(h).wait()
        v_copy(h).wait()
        p = jnp.exp2((fresh_scores[lax.rem(h, 2)] - full_max[...]) * EXP2_SCALE)
        part_sum[...] = p
        acc[...] = jnp.dot(
            p.astype(jnp.bfloat16), fvbuf[h], preferred_element_type=jnp.float32
        )

    def values_block(h, c):
        top = full_max[...]
        total = part_sum[...]
        pieces = []
        for i in range(block // LANES):
            s = scores[lax.rem(h, 2), c, :, i * LANES:(i + 1) * LANES]
            p = jnp.exp2((s - top) * EXP2_SCALE)
            total = total + p
            pieces.append(p.astype(jnp.bfloat16))
        part_sum[...] = total
        values = vbuf[h, pl.ds(pl.multiple_of(c * block, block), block), :]
        acc[...] += jnp.dot(
            jnp.concatenate(pieces, axis=1), values, preferred_element_type=jnp.float32
        )

    lane = lax.broadcasted_iota(jnp.int32, (each, LANES), 1)
    sub = lax.broadcasted_iota(jnp.int32, (each, LANES), 0)

    def o_copy(h, slot):
        peer = lax.rem(slot, pairs) * 2 + lax.div(slot, pairs)
        return pltpu.make_async_remote_copy(
            src_ref=obuf.at[h, slot], dst_ref=rbuf.at[h, my_slot],
            send_sem=o_send.at[h], recv_sem=o_recv.at[h],
            device_id={"ctx": peer}, device_id_type=pl.DeviceIdType.MESH,
        )

    def ml_copy(h, slot):
        peer = lax.rem(slot, pairs) * 2 + lax.div(slot, pairs)
        return pltpu.make_async_remote_copy(
            src_ref=mlbuf.at[h, slot], dst_ref=rmlbuf.at[h, my_slot],
            send_sem=ml_send.at[h], recv_sem=ml_recv.at[h],
            device_id={"ctx": peer}, device_id_type=pl.DeviceIdType.MESH,
        )

    def values_close(h):
        total = jnp.sum(part_sum[...], axis=1, keepdims=True)
        out = (acc[...] / total).astype(jnp.bfloat16)
        obuf[h] = out.reshape(devices, each, HEAD_SIZE)
        for slot in range(devices):
            span = slice(slot * each, (slot + 1) * each)
            tops = jnp.where(lane == sub, full_max[span, :], 0.0)
            sums = jnp.where(lane == sub + each, jnp.broadcast_to(total[span], tops.shape), 0.0)
            mlbuf[h, slot] = jnp.sum(tops + sums, axis=0, keepdims=True)
        rbuf[h, my_slot] = obuf[h, my_slot]
        rmlbuf[h, my_slot] = mlbuf[h, my_slot]

    def send_out(h):
        def send(step, _):
            slot = lax.rem(my_slot + step, devices)
            ml_copy(h, slot).start()
            o_copy(h, slot).start()
            return 0

        lax.fori_loop(1, devices, send, 0)

    def o_blocks(ref, h, sem):
        blocks = ref.at[h, pl.ds(0, devices - 1)]
        return pltpu.make_async_copy(blocks, blocks, sem.at[h])

    def combine(h):
        o_blocks(rmlbuf, h, ml_recv).wait()
        o_blocks(rbuf, h, o_recv).wait()
        ml = rmlbuf[h, :, 0, :]
        tops, sums = ml[:, :each], ml[:, each:2 * each]
        weights = jnp.exp2((tops - jnp.max(tops, axis=0, keepdims=True)) * EXP2_SCALE) * sums
        weights = weights / jnp.sum(weights, axis=0, keepdims=True)
        diagonal = lax.broadcasted_iota(jnp.int32, (each, each), 0) == lax.broadcasted_iota(
            jnp.int32, (each, each), 1
        )
        result = jnp.zeros((each, HEAD_SIZE), jnp.float32)
        for slot in range(devices):
            row = jnp.broadcast_to(weights[slot:slot + 1, :], (each, each))
            column = jnp.sum(jnp.where(diagonal, row, 0.0), axis=1, keepdims=True)
            result = result + column * rbuf[h, slot].astype(jnp.float32)
        for g in range(group):
            columns = pl.ds(pl.multiple_of((h * group + g) * HEAD_SIZE, HEAD_SIZE), HEAD_SIZE)
            out_ref[:, columns] = result[g * own:(g + 1) * own].astype(out_ref.dtype)

    def loop(body):
        def step(c, _):
            body(c)
            return 0

        lax.fori_loop(0, count, step, 0)

    lag = 3
    relay(0)
    if heads > 1:
        relay(1)
    scores_open(0)
    loop(lambda c: scores_block(0, c))
    scores_close()

    def head_step(h, _):
        @pl.when(h + 1 < heads)
        def _():
            relay(h + 1)

        values_open(h - 1)
        scores_open(h)

        def both(c):
            values_block(h - 1, c)
            scores_block(h, c)

        loop(both)
        values_close(h - 1)
        scores_close()
        send_out(h - 1)

        @pl.when(h > lag)
        def _():
            combine(h - 1 - lag)

        return 0

    lax.fori_loop(1, heads, head_step, 0)
    last = heads - 1
    values_open(last)
    loop(lambda c: values_block(last, c))
    values_close(last)
    send_out(last)
    lax.fori_loop(max(0, heads - 1 - lag), heads, lambda h, _: (combine(h), 0)[1], 0)

    def drain(h, _):
        gather_blocks(h, gather_send).wait()
        relay_copy(h).wait_send()
        o_blocks(mlbuf, h, ml_send).wait()
        o_blocks(obuf, h, o_send).wait()
        return 0

    lax.fori_loop(0, heads, drain, 0)


def solution(mesh):
    devices = mesh.shape["ctx"]

    def shards(queries, cache_keys, prefix_values, incoming_keys, incoming_values):
        own = queries.shape[0]
        heads = cache_keys.shape[1] // HEAD_SIZE
        group = queries.shape[1] // cache_keys.shape[1]
        depth = cache_keys.shape[0]
        each = group * own
        rows = devices * each
        block = min(BLOCK_KEYS, depth)
        bf16, f32 = jnp.bfloat16, jnp.float32
        dma = pltpu.SemaphoreType.DMA
        return pl.pallas_call(
            functools.partial(kernel, devices, heads, group, own, block),
            out_shape=jax.ShapeDtypeStruct(queries.shape, queries.dtype),
            in_specs=[pl.BlockSpec(memory_space=pl.ANY)] * 5,
            out_specs=pl.BlockSpec(memory_space=pltpu.VMEM),
            scratch_shapes=[
                pltpu.VMEM((heads, 2, devices // 2, each, HEAD_SIZE), bf16),
                pltpu.VMEM((heads, depth, HEAD_SIZE), bf16),
                pltpu.VMEM((heads, depth, HEAD_SIZE), bf16),
                pltpu.VMEM((heads, LANES, HEAD_SIZE), bf16),
                pltpu.VMEM((heads, LANES, HEAD_SIZE), bf16),
                pltpu.VMEM((2, depth // block, rows, block), f32),
                pltpu.VMEM((2, rows, LANES), f32),
                pltpu.VMEM((rows, LANES), f32),
                pltpu.VMEM((rows, LANES), f32),
                pltpu.VMEM((rows, LANES), f32),
                pltpu.VMEM((rows, LANES), f32),
                pltpu.VMEM((rows, HEAD_SIZE), f32),
                pltpu.VMEM((heads, devices, each, HEAD_SIZE), bf16),
                pltpu.VMEM((heads, devices, each, HEAD_SIZE), bf16),
                pltpu.VMEM((heads, devices, 1, LANES), f32),
                pltpu.VMEM((heads, devices, 1, LANES), f32),
                dma((heads, group)), dma((heads,)), dma((heads,)), dma((heads,)), dma((heads,)),
                dma((heads,)), dma((heads,)), dma((heads,)), dma((heads,)),
                dma((heads,)), dma((heads,)), dma((heads,)), dma((heads,)),
            ],
            compiler_params=pltpu.CompilerParams(
                collective_id=0, has_side_effects=True, vmem_limit_bytes=60 * 1024 * 1024
            ),
        )(queries, cache_keys, prefix_values, incoming_keys, incoming_values)

    spec = P("ctx", "head")
    return jax.shard_map(
        shards, mesh=mesh, in_specs=(spec,) * 5, out_specs=spec, check_vma=False
    )
```

```python
import functools
import math

import jax
import jax.numpy as jnp
from jax import lax
from jax.experimental import pallas as pl
from jax.experimental.pallas import tpu as pltpu
from jax.sharding import PartitionSpec as P

HEAD_SIZE = 128
LANES = 128
BLOCK_KEYS = 2048
EXP2_SCALE = 168.0 ** (-0.5) * math.log2(math.e)
MASKED = -1e30


def nt_dot(a, b):
    return lax.dot_general(a, b, (((1,), (1,)), ((), ())), preferred_element_type=jnp.float32)


def kernel(
    devices, heads, group, own, block,
    q_hbm, k_hbm, v_hbm, fk_hbm, fv_hbm, out_ref,
    qbuf, kbuf, vbuf, fkbuf, fvbuf, scores_even, scores_odd, fresh_scores, visible,
    part_max, full_max, part_sum, acc, obuf, rbuf, mlbuf, rmlbuf,
    q_sem, k_sem, v_sem, fk_sem, fv_sem,
    gather_send, gather_recv, relay_send, relay_recv,
    o_send, o_recv, ml_send, ml_recv,
):
    pairs = devices // 2
    each = group * own
    rows = devices * each
    count = kbuf.shape[1] // block
    me = lax.axis_index("ctx")
    core, pair = lax.rem(me, 2), lax.div(me, 2)
    my_slot = core * pairs + pair

    def q_copy(h, g):
        columns = pl.ds((h * group + g) * HEAD_SIZE, HEAD_SIZE)
        return pltpu.make_async_copy(
            q_hbm.at[:, columns], qbuf.at[h, core, pair, pl.ds(g * own, own)], q_sem.at[h, g]
        )

    def head_columns(h):
        return pl.ds(pl.multiple_of(h * HEAD_SIZE, HEAD_SIZE), HEAD_SIZE)

    def k_copy(h):
        return pltpu.make_async_copy(k_hbm.at[:, head_columns(h)], kbuf.at[h], k_sem.at[h])

    def v_copy(h):
        return pltpu.make_async_copy(v_hbm.at[:, head_columns(h)], vbuf.at[h], v_sem.at[h])

    def fk_copy(h):
        return pltpu.make_async_copy(
            fk_hbm.at[:, head_columns(h)], fkbuf.at[h, pl.ds(0, own)], fk_sem.at[h]
        )

    def fv_copy(h):
        return pltpu.make_async_copy(
            fv_hbm.at[:, head_columns(h)], fvbuf.at[h, pl.ds(0, own)], fv_sem.at[h]
        )

    for h in range(heads):
        for g in range(group):
            q_copy(h, g).start()

    barrier = pltpu.get_barrier_semaphore()

    def greet(step, _):
        peer = lax.rem(me + step, devices)
        pl.semaphore_signal(
            barrier, inc=1, device_id={"ctx": peer}, device_id_type=pl.DeviceIdType.MESH
        )
        return 0

    lax.fori_loop(1, devices, greet, 0)
    fkbuf[:, own:, :] = jnp.zeros((heads, LANES - own, HEAD_SIZE), fkbuf.dtype)
    fvbuf[:, own:, :] = jnp.zeros((heads, LANES - own, HEAD_SIZE), fvbuf.dtype)
    for h in range(heads):
        fk_copy(h).start()
        k_copy(h).start()
        fv_copy(h).start()
        v_copy(h).start()

    key_lane = lax.broadcasted_iota(jnp.int32, (own, LANES), 1)
    key_pos = me * own + key_lane
    token = lax.broadcasted_iota(jnp.int32, (own, LANES), 0)
    for slot in range(devices):
        device = (slot % pairs) * 2 + slot // pairs
        seen = jnp.where((key_lane < own) & (key_pos <= device * own + token), 0.0, MASKED)
        for g in range(group):
            visible[pl.ds(slot * each + g * own, own), :] = seen

    for h in range(heads):
        for g in range(group):
            q_copy(h, g).wait()
    pl.semaphore_wait(barrier, devices - 1)

    def gather_copy(h, peer_pair):
        mine = qbuf.at[h, core, pair]
        return pltpu.make_async_remote_copy(
            src_ref=mine, dst_ref=mine, send_sem=gather_send.at[h], recv_sem=gather_recv.at[h],
            device_id={"ctx": peer_pair * 2 + core}, device_id_type=pl.DeviceIdType.MESH,
        )

    def gather_head(h, _):
        def send(step, _):
            gather_copy(h, lax.rem(pair + step, pairs)).start()
            return 0

        return lax.fori_loop(1, pairs, send, 0)

    lax.fori_loop(0, heads, gather_head, 0)

    def relay_copy(h):
        mine = qbuf.at[h, core]
        return pltpu.make_async_remote_copy(
            src_ref=mine, dst_ref=mine, send_sem=relay_send.at[h], recv_sem=relay_recv.at[h],
            device_id={"ctx": pair * 2 + 1 - core}, device_id_type=pl.DeviceIdType.MESH,
        )

    def gather_blocks(h, sem):
        blocks = qbuf.at[h, core, pl.ds(0, pairs - 1)]
        return pltpu.make_async_copy(blocks, blocks, sem.at[h])

    def relay(h):
        gather_blocks(h, gather_recv).wait()
        relay_copy(h).start()

    def queries_of(h):
        return qbuf[h].reshape(rows, HEAD_SIZE)

    score_slots = (scores_even, scores_odd)

    def scores_open(h):
        relay_copy(h).wait_recv()
        fk_copy(h).wait()
        k_copy(h).wait()
        s = nt_dot(queries_of(h), fkbuf[h]) + visible[...]
        s = jnp.where(visible[...] < 0.0, MASKED, s)
        fresh_scores[lax.rem(h, 2)] = s
        part_max[...] = s

    def scores_block(h, c, parity):
        keys = kbuf[h, pl.ds(pl.multiple_of(c * block, block), block), :]
        s = nt_dot(queries_of(h), keys)
        score_slots[parity][c] = s
        top = part_max[...]
        for i in range(block // LANES):
            top = jnp.maximum(top, s[:, i * LANES:(i + 1) * LANES])
        part_max[...] = top

    def scores_close():
        full_max[...] = jnp.broadcast_to(
            jnp.max(part_max[...], axis=1, keepdims=True), full_max.shape
        )

    def values_open(h):
        fv_copy(h).wait()
        v_copy(h).wait()
        p = jnp.exp2((fresh_scores[lax.rem(h, 2)] - full_max[...]) * EXP2_SCALE)
        part_sum[...] = p
        acc[...] = jnp.dot(
            p.astype(jnp.bfloat16), fvbuf[h], preferred_element_type=jnp.float32
        )

    def values_block(h, c, parity):
        top = full_max[...]
        total = part_sum[...]
        pieces = []
        for i in range(block // LANES):
            s = score_slots[parity][c, :, i * LANES:(i + 1) * LANES]
            p = jnp.exp2((s - top) * EXP2_SCALE)
            total = total + p
            pieces.append(p.astype(jnp.bfloat16))
        part_sum[...] = total
        values = vbuf[h, pl.ds(pl.multiple_of(c * block, block), block), :]
        acc[...] += jnp.dot(
            jnp.concatenate(pieces, axis=1), values, preferred_element_type=jnp.float32
        )

    lane = lax.broadcasted_iota(jnp.int32, (each, LANES), 1)
    sub = lax.broadcasted_iota(jnp.int32, (each, LANES), 0)

    def o_copy(h, slot):
        peer = lax.rem(slot, pairs) * 2 + lax.div(slot, pairs)
        return pltpu.make_async_remote_copy(
            src_ref=obuf.at[h, slot], dst_ref=rbuf.at[h, my_slot],
            send_sem=o_send.at[h], recv_sem=o_recv.at[h],
            device_id={"ctx": peer}, device_id_type=pl.DeviceIdType.MESH,
        )

    def ml_copy(h, slot):
        peer = lax.rem(slot, pairs) * 2 + lax.div(slot, pairs)
        return pltpu.make_async_remote_copy(
            src_ref=mlbuf.at[h, slot], dst_ref=rmlbuf.at[h, my_slot],
            send_sem=ml_send.at[h], recv_sem=ml_recv.at[h],
            device_id={"ctx": peer}, device_id_type=pl.DeviceIdType.MESH,
        )

    def values_close(h):
        total = jnp.sum(part_sum[...], axis=1, keepdims=True)
        out = (acc[...] / total).astype(jnp.bfloat16)
        obuf[h] = out.reshape(devices, each, HEAD_SIZE)
        for slot in range(devices):
            span = slice(slot * each, (slot + 1) * each)
            tops = jnp.where(lane == sub, full_max[span, :], 0.0)
            sums = jnp.where(lane == sub + each, jnp.broadcast_to(total[span], tops.shape), 0.0)
            mlbuf[h, slot] = jnp.sum(tops + sums, axis=0, keepdims=True)
        rbuf[h, my_slot] = obuf[h, my_slot]
        rmlbuf[h, my_slot] = mlbuf[h, my_slot]

    def send_out(h):
        def send(step, _):
            slot = lax.rem(my_slot + step, devices)
            ml_copy(h, slot).start()
            o_copy(h, slot).start()
            return 0

        lax.fori_loop(1, devices, send, 0)

    def o_blocks(ref, h, sem):
        blocks = ref.at[h, pl.ds(0, devices - 1)]
        return pltpu.make_async_copy(blocks, blocks, sem.at[h])

    def combine(h):
        o_blocks(rmlbuf, h, ml_recv).wait()
        o_blocks(rbuf, h, o_recv).wait()
        ml = rmlbuf[h, :, 0, :]
        tops, sums = ml[:, :each], ml[:, each:2 * each]
        weights = jnp.exp2((tops - jnp.max(tops, axis=0, keepdims=True)) * EXP2_SCALE) * sums
        weights = weights / jnp.sum(weights, axis=0, keepdims=True)
        diagonal = lax.broadcasted_iota(jnp.int32, (each, each), 0) == lax.broadcasted_iota(
            jnp.int32, (each, each), 1
        )
        result = jnp.zeros((each, HEAD_SIZE), jnp.float32)
        for slot in range(devices):
            row = jnp.broadcast_to(weights[slot:slot + 1, :], (each, each))
            column = jnp.sum(jnp.where(diagonal, row, 0.0), axis=1, keepdims=True)
            result = result + column * rbuf[h, slot].astype(jnp.float32)
        for g in range(group):
            columns = pl.ds(pl.multiple_of((h * group + g) * HEAD_SIZE, HEAD_SIZE), HEAD_SIZE)
            out_ref[:, columns] = result[g * own:(g + 1) * own].astype(out_ref.dtype)

    def loop(body):
        def step(c, _):
            body(c)
            return 0

        lax.fori_loop(0, count, step, 0)

    lag = 3
    relay(0)
    if heads > 1:
        relay(1)
    scores_open(0)
    loop(lambda c: scores_block(0, c, 0))
    scores_close()

    def head_step(h, parity):
        @pl.when(h + 1 < heads)
        def _():
            relay(h + 1)

        values_open(h - 1)
        scores_open(h)

        def both(c):
            values_block(h - 1, c, 1 - parity)
            scores_block(h, c, parity)

        loop(both)
        values_close(h - 1)
        scores_close()
        send_out(h - 1)

        @pl.when(h > lag)
        def _():
            combine(h - 1 - lag)

    def two_heads(step, _):
        head_step(1 + 2 * step, 1)
        head_step(2 + 2 * step, 0)
        return 0

    lax.fori_loop(0, (heads - 1) // 2, two_heads, 0)
    if heads % 2 == 0:
        head_step(heads - 1, 1)
    last = heads - 1
    values_open(last)
    loop(lambda c: values_block(last, c, last % 2))
    values_close(last)
    send_out(last)
    lax.fori_loop(max(0, heads - 1 - lag), heads, lambda h, _: (combine(h), 0)[1], 0)

    def drain(h, _):
        gather_blocks(h, gather_send).wait()
        relay_copy(h).wait_send()
        o_blocks(mlbuf, h, ml_send).wait()
        o_blocks(obuf, h, o_send).wait()
        return 0

    lax.fori_loop(0, heads, drain, 0)


def solution(mesh):
    devices = mesh.shape["ctx"]

    def shards(queries, cache_keys, prefix_values, incoming_keys, incoming_values):
        own = queries.shape[0]
        heads = cache_keys.shape[1] // HEAD_SIZE
        group = queries.shape[1] // cache_keys.shape[1]
        depth = cache_keys.shape[0]
        each = group * own
        rows = devices * each
        block = min(BLOCK_KEYS, depth)
        bf16, f32 = jnp.bfloat16, jnp.float32
        dma = pltpu.SemaphoreType.DMA
        return pl.pallas_call(
            functools.partial(kernel, devices, heads, group, own, block),
            out_shape=jax.ShapeDtypeStruct(queries.shape, queries.dtype),
            in_specs=[pl.BlockSpec(memory_space=pl.ANY)] * 5,
            out_specs=pl.BlockSpec(memory_space=pltpu.VMEM),
            scratch_shapes=[
                pltpu.VMEM((heads, 2, devices // 2, each, HEAD_SIZE), bf16),
                pltpu.VMEM((heads, depth, HEAD_SIZE), bf16),
                pltpu.VMEM((heads, depth, HEAD_SIZE), bf16),
                pltpu.VMEM((heads, LANES, HEAD_SIZE), bf16),
                pltpu.VMEM((heads, LANES, HEAD_SIZE), bf16),
                pltpu.VMEM((depth // block, rows, block), f32),
                pltpu.VMEM((depth // block, rows, block), f32),
                pltpu.VMEM((2, rows, LANES), f32),
                pltpu.VMEM((rows, LANES), f32),
                pltpu.VMEM((rows, LANES), f32),
                pltpu.VMEM((rows, LANES), f32),
                pltpu.VMEM((rows, LANES), f32),
                pltpu.VMEM((rows, HEAD_SIZE), f32),
                pltpu.VMEM((heads, devices, each, HEAD_SIZE), bf16),
                pltpu.VMEM((heads, devices, each, HEAD_SIZE), bf16),
                pltpu.VMEM((heads, devices, 1, LANES), f32),
                pltpu.VMEM((heads, devices, 1, LANES), f32),
                dma((heads, group)), dma((heads,)), dma((heads,)), dma((heads,)), dma((heads,)),
                dma((heads,)), dma((heads,)), dma((heads,)), dma((heads,)),
                dma((heads,)), dma((heads,)), dma((heads,)), dma((heads,)),
            ],
            compiler_params=pltpu.CompilerParams(
                collective_id=0, has_side_effects=True, vmem_limit_bytes=60 * 1024 * 1024
            ),
        )(queries, cache_keys, prefix_values, incoming_keys, incoming_values)

    spec = P("ctx", "head")
    return jax.shard_map(
        shards, mesh=mesh, in_specs=(spec,) * 5, out_specs=spec, check_vma=False
    )
```
